512 devices in a mesh: tp: 8 (over y), row: 8 (over z_hi, x), col: 8 (over z_lo, core).
Axes of the slice: x: 4, y: 8, z: 8 (z_hi: 2, z_lo: 4; z = z_hi * 4 + z_lo), core: 2. Of those that a mesh axis runs over, the one named last changes fastest.
Arguments:
- hidden: bfloat16 [128, 14336], P('col', 'row'), may hold values from -6 to 6
- out_grad: bfloat16 [128, 4096], P(None, ('tp', 'row')), may hold values from -6 to 6
- basis_in: bfloat16 [14336, 4096], P(('row', 'col'), 'tp'), may hold values from -0.046875 to 0.046875
- basis_out: bfloat16 [4096, 1024], P(('tp', 'row'), 'col'), may hold values from -0.09375 to 0.09375
- eigen: float32 [4096, 1024], P(('tp', 'row'), 'col'), may hold values from 0.02 to 2
Outputs:
- precond: float32 [4096, 14336], P(('tp', 'col'), 'row')
The draws below stay inside these ranges and needn't reach their ends.
All inputs are finite; a program needn't handle non-finite values.
Results may differ from the reference program's by a relative error of at most 0.024.
Values may be sent and summed in bfloat16 or wider, within the bound.
A program may use at most 64 MiB of HBM per device.

```python
import math
import jax
import jax.numpy as jnp
from jax import lax

D = 4096
FF = 14336
KIN = 4096
KOUT = 1024
TQ = 128
N_TP = 8
N_COL = 8


def block_scale(rng, shape, shards, smallest, largest):
    level = 1.0
    for dim, shards_of in shards:
        heights = jax.random.uniform(jax.random.fold_in(jax.random.fold_in(rng, 6), dim), (shards_of,), jnp.float32, smallest / len(shards), largest / len(shards))
        level = level * jnp.repeat(jnp.exp(heights), shape[dim] // shards_of).reshape((-1,) + (1,) * (len(shape) - 1 - dim))
    return level


def centred(own_key, extent, scale, bound, pieces=(), held_as=jnp.bfloat16):
    array = jax.random.normal(own_key, extent, jnp.float32) * scale
    if len(pieces) > 0:
        array = block_scale(own_key, extent, pieces, -0.22, 0.18) * array
    return jnp.clip(array, min=-bound, max=bound).astype(held_as)


def setup_inputs(seed: int = 0) -> dict:
    seeds = jax.random.split(jax.random.key(seed), 6)
    hidden = centred(seeds[0], (TQ, FF), 1.0, 6.0, ((0, 8), (1, 8)))
    out_grad = centred(seeds[1], (TQ, D), 1.0, 6.0, ((1, 64),))
    basis_in = centred(seeds[2], (FF, KIN), FF ** -0.5, 0.046875, ((0, 64), (1, 8)))
    basis_out = centred(seeds[3], (D, KOUT), D ** -0.5, 0.09375, ((0, 64), (1, 8)))
    eigen = jnp.clip(jnp.exp(math.log(2.0) - 4.6051702 * jax.random.uniform(seeds[4], (KIN, KOUT), jnp.float32) ** block_scale(seeds[4], (KIN, KOUT), ((0, 64), (1, 8)), -0.2, 0.2)), 0.02, 2.0)
    return {"hidden": hidden, "out_grad": out_grad, "basis_in": basis_in, "basis_out": basis_out, "eigen": eigen}


damping = 0.01


def reference(hidden, out_grad, basis_in, basis_out, eigen):
    rot_in = jnp.dot(hidden, basis_in, preferred_element_type=jnp.float32).astype(jnp.bfloat16)
    rot_out = jnp.dot(out_grad, basis_out, preferred_element_type=jnp.float32).astype(jnp.bfloat16)
    coeff = jnp.dot(rot_out.T, rot_in, preferred_element_type=jnp.float32)
    scaled = (coeff / (TQ * (eigen.T + damping))).astype(jnp.bfloat16)
    out_block = KOUT // N_COL
    mixed = jnp.zeros((D, KIN), jnp.float32)
    for index in range(N_COL):
        part = jnp.dot(basis_out[:, index * out_block:(index + 1) * out_block], scaled[index * out_block:(index + 1) * out_block], preferred_element_type=jnp.float32)
        part = lax.optimization_barrier(part.astype(jnp.bfloat16))
        mixed = mixed + part.astype(jnp.float32)
    mixed = mixed.astype(jnp.bfloat16)
    in_block = KIN // N_TP
    result = jnp.zeros((D, FF), jnp.float32)
    for index in range(N_TP):
        part = jnp.dot(mixed[:, index * in_block:(index + 1) * in_block], basis_in[:, index * in_block:(index + 1) * in_block].T, preferred_element_type=jnp.float32)
        part = lax.optimization_barrier(part.astype(jnp.bfloat16))
        result = result + part.astype(jnp.float32)
    return result
```

```python
import functools

import jax
import jax.numpy as jnp
from jax import lax
from jax.experimental import pallas as pl
from jax.experimental.pallas import tpu as pltpu
from jax.sharding import PartitionSpec as P

MESH = pl.DeviceIdType.MESH
BF16 = jnp.bfloat16
F32 = jnp.float32
damping = 0.01
NX, NZ_HI, NZ_LO, NC = 4, 2, 4, 2
NZ = NZ_HI * NZ_LO
NY = 8
SPLIT = 2


def far_first(count):
    return sorted(range(1, count), key=lambda hop: -min(hop, count - hop))


def kernel(
    hidden, out_grad, basis_in, basis_out, eigen, out,
    hid_v, grad_v, eig_v, basis, hid_s, hid_r,
    p_s, p_r, p_x, p_g, rin,
    r_s, r_r, r_y, r_z, r_x,
    e_g, b_g, scaled, w_s, w_1, w_2, w_g, b_full, o_f, o_s, o_r, f_s, f_r,
    load_sem, send_sem, recv_sem,
):
    t = lax.axis_index("tp")
    row = lax.axis_index("row")
    col = lax.axis_index("col")
    z_hi, x = lax.div(row, NX), lax.rem(row, NX)
    z_lo, core = lax.div(col, NC), lax.rem(col, NC)
    z = z_hi * NZ_LO + z_lo

    def at_y(pos):
        return {"tp": pos}

    def at_x(pos):
        return {"row": z_hi * NX + pos}

    def at_z(pos):
        return {
            "row": lax.div(pos, NZ_LO) * NX + x,
            "col": lax.rem(pos, NZ_LO) * NC + core,
        }

    def at_zlo(pos):
        return {"col": pos * NC + core}

    at_core = {"col": z_lo * NC + 1 - core}

    slots = [0]
    sent = []

    def fresh(count):
        first = slots[0]
        slots[0] += count
        return first

    def remote(src, dst, sem, device):
        return pltpu.make_async_remote_copy(
            src_ref=src, dst_ref=dst, send_sem=send_sem.at[sem], recv_sem=recv_sem.at[sem],
            device_id=device, device_id_type=MESH,
        )

    def start(src, dst, sem, device):
        copy = remote(src, dst, sem, device)
        copy.start()
        sent.append(copy)

    def exchange(src, dst, me, count, at):
        first = fresh(count)
        for hop in far_first(count):
            peer = lax.rem(me + hop, count)
            start(src(peer), dst(me), first + hop, at(peer))

        def finish():
            for hop in reversed(far_first(count)):
                sender = lax.rem(me + count - hop, count)
                remote(src(sender), dst(sender), first + hop, at(sender)).wait_recv()

        return finish

    def gather(buf, me, count, at):
        return exchange(lambda peer: buf.at[me], lambda sender: buf.at[sender], me, count, at)

    def scatter(src, dst, me, count, at):
        return exchange(lambda peer: src.at[peer], lambda sender: dst.at[sender], me, count, at)

    def total(buf, count):
        acc = buf[0].astype(F32)
        for i in range(1, count):
            acc = acc + buf[i].astype(F32)
        return acc

    def put(buf, pos, value):
        buf[pl.ds(pos, 1)] = value[None]

    loads = [
        pltpu.make_async_copy(hidden, hid_v, load_sem.at[0]),
        pltpu.make_async_copy(out_grad, grad_v, load_sem.at[1]),
        pltpu.make_async_copy(basis_out, b_g.at[x, z], load_sem.at[2]),
        pltpu.make_async_copy(basis_in, basis.at[core], load_sem.at[3]),
        pltpu.make_async_copy(eigen, eig_v, load_sem.at[4]),
    ]
    for load in loads:
        load.start()

    barrier = pltpu.get_barrier_semaphore()
    partners = [at_core]
    partners += [at_x(lax.rem(x + hop, NX)) for hop in range(1, NX)]
    partners += [at_z(lax.rem(z + hop, NZ)) for hop in range(1, NZ)]
    partners += [at_y(lax.rem(t + hop, NY)) for hop in range(1, NY)]
    for partner in partners:
        pl.semaphore_signal(barrier, inc=1, device_id=partner, device_id_type=MESH)

    own_tok = hid_v.shape[0]
    wide = hid_s.shape[2]
    loads[0].wait()
    hid = hid_v[...]
    for i in range(NZ_LO):
        hid_s[i] = hid[:, i * wide:(i + 1) * wide]
    hid_r[pl.ds(z_lo, 1)] = hid_s[pl.ds(z_lo, 1)]

    loads[1].wait()
    loads[2].wait()
    part = jnp.dot(grad_v[...], b_g[x, z], preferred_element_type=F32)
    order = [i * NC + p for p in range(NC) for i in range(NZ_LO)]
    part = jnp.concatenate([part[i * own_tok:(i + 1) * own_tok] for i in order], axis=0)
    piece = r_s.shape[1]
    for i in range(NX):
        r_s[i] = part[i * piece:(i + 1) * piece].astype(BF16)
    r_r[pl.ds(x, 1)] = r_s[pl.ds(x, 1)]
    loads[3].wait()
    loads[4].wait()
    queries = own_tok * NZ_LO * NC
    e_g[x, z] = (1.0 / (queries * (eig_v[...] + damping))).astype(BF16)

    pl.semaphore_wait(barrier, len(partners))

    hid_done = scatter(hid_s, hid_r, z_lo, NZ_LO, at_zlo)
    basis_sem = fresh(1)
    start(basis.at[core], basis.at[core], basis_sem, at_core)
    r_done = scatter(r_s, r_r, x, NX, at_x)
    ez_done = exchange(
        lambda peer: e_g.at[x, z], lambda sender: e_g.at[x, sender], z, NZ, at_z
    )

    r_done()
    put(r_y, t, total(r_r, NX).astype(BF16))
    ry_done = gather(r_y, t, NY, at_y)

    hid_done()
    remote(basis.at[core], basis.at[1 - core], basis_sem, at_core).wait_recv()
    deep = NC * basis.shape[1]
    basis_rows = basis[...].reshape(deep, basis.shape[2])
    p_full = jnp.dot(
        hid_r[...].reshape(NZ_LO * own_tok, wide), basis_rows, preferred_element_type=F32
    )
    tall, broad = p_s.shape[1:]
    across = basis.shape[2] // broad
    for i in range(NZ):
        h, q = i // across, i % across
        p_s[i] = p_full[h * tall:(h + 1) * tall, q * broad:(q + 1) * broad].astype(BF16)
    p_r[pl.ds(z, 1)] = p_s[pl.ds(z, 1)]
    p_done = scatter(p_s, p_r, z, NZ, at_z)

    ry_done()
    put(r_z, z, total(r_y, NY).astype(BF16))
    rz_done = gather(r_z, z, NZ, at_z)

    p_done()
    put(p_x, x, total(p_r, NZ).astype(BF16))
    px_done = gather(p_x, x, NX, at_x)

    ez_done()
    ex_done = gather(e_g, x, NX, at_x)

    px_done()
    put(p_g, z, total(p_x, NX).astype(BF16))
    pg_done = gather(p_g, z, NZ, at_z)

    rz_done()
    put(
        r_x, x,
        jnp.concatenate(
            [
                sum(r_z[h * NZ_LO + i].astype(F32) for h in range(NZ_HI)).astype(BF16)
                for i in range(NZ_LO)
            ],
            axis=1,
        ),
    )
    rx_done = gather(r_x, x, NX, at_x)

    pg_done()
    put(
        rin, core,
        jnp.concatenate(
            [
                jnp.concatenate([p_g[h * across + q] for q in range(across)], axis=1)
                for h in range(NZ // across)
            ],
            axis=0,
        ),
    )
    rin_sem = fresh(1)
    start(rin.at[core], rin.at[core], rin_sem, at_core)
    bz_done = exchange(
        lambda peer: b_g.at[x, z], lambda sender: b_g.at[x, sender], z, NZ, at_z
    )

    rx_done()
    remote(rin.at[core], rin.at[1 - core], rin_sem, at_core).wait_recv()
    depth = basis.shape[2]
    across_out = NZ_LO * b_g.shape[3]
    coeff = lax.dot_general(
        rin[...].reshape(queries, depth), r_x[...].reshape(queries, across_out),
        (((0,), (0,)), ((), ())), preferred_element_type=F32,
    )
    ex_done()
    rows, cols = b_g.shape[2:]
    for i in range(NX):
        for k in range(NZ):
            h, low = k // NZ_LO, k % NZ_LO
            r0, c0 = (h * NX + i) * rows, low * cols
            scaled[r0:r0 + rows, c0:c0 + cols] = (
                coeff[r0:r0 + rows, c0:c0 + cols] * e_g[i, k].astype(F32)
            ).astype(BF16)

    w_full = jnp.dot(basis_rows, scaled[...], preferred_element_type=F32)
    chunk = w_s.shape[1]
    for i in range(NY):
        w_s[i] = w_full[i * chunk:(i + 1) * chunk].astype(BF16)

    heading = 1 - 2 * core
    ahead = at_y(lax.rem(t + heading + NY, NY))
    behind = at_y(lax.rem(t - heading + NY, NY))
    first_hops, second_hops = NY // 2, NY // 2 - 1
    span = w_s.shape[2] // SPLIT

    def off(steps):
        return lax.rem(t + heading * steps + 2 * NY, NY)

    def cut(buf, slot, q):
        return buf.at[slot, :, pl.ds(q * span, span)]

    def add_in(slot, buf, step, q):
        here = (pl.ds(slot, 1), slice(None), pl.ds(q * span, span))
        there = (pl.ds(step, 1), slice(None), pl.ds(q * span, span))
        w_s[here] = (w_s[here].astype(F32) + buf[there].astype(F32)).astype(BF16)

    sem_1 = fresh(first_hops * SPLIT)
    sem_2 = fresh(second_hops * SPLIT)
    for step in range(first_hops):
        for q in range(SPLIT):
            dest = off(first_hops - step)
            sem = sem_1 + step * SPLIT + q
            if step > 0:
                remote(cut(w_s, dest, q), cut(w_1, step - 1, q), sem - SPLIT, behind).wait_recv()
                add_in(dest, w_1, step - 1, q)
            start(cut(w_s, dest, q), cut(w_1, step, q), sem, ahead)
            if step < second_hops:
                dest = off(step - second_hops)
                sem = sem_2 + step * SPLIT + q
                if step > 0:
                    remote(cut(w_s, dest, q), cut(w_2, step - 1, q), sem - SPLIT, ahead).wait_recv()
                    add_in(dest, w_2, step - 1, q)
                start(cut(w_s, dest, q), cut(w_2, step, q), sem, behind)

    bz_done()
    bx_done = gather(b_g, x, NX, at_x)

    gsem_1 = fresh(first_hops * SPLIT)
    gsem_2 = fresh(second_hops * SPLIT)
    for q in range(SPLIT):
        remote(
            cut(w_s, t, q), cut(w_2, second_hops - 1, q),
            sem_2 + (second_hops - 1) * SPLIT + q, ahead,
        ).wait_recv()
        add_in(t, w_2, second_hops - 1, q)
        remote(
            cut(w_s, t, q), cut(w_1, first_hops - 1, q),
            sem_1 + (first_hops - 1) * SPLIT + q, behind,
        ).wait_recv()
        here = (pl.ds(t, 1), slice(None), pl.ds(q * span, span))
        w_g[here] = (
            w_s[here].astype(F32) + w_1[first_hops - 1, :, q * span:(q + 1) * span].astype(F32)[None]
        ).astype(BF16)
        start(cut(w_g, t, q), cut(w_g, t, q), gsem_1 + q, ahead)
        start(cut(w_g, t, q), cut(w_g, t, q), gsem_2 + q, behind)
    for step in range(1, first_hops + 1):
        for q in range(SPLIT):
            slot = off(-step)
            sem = gsem_1 + step * SPLIT + q
            remote(cut(w_g, slot, q), cut(w_g, slot, q), sem - SPLIT, behind).wait_recv()
            if step < first_hops:
                start(cut(w_g, slot, q), cut(w_g, slot, q), sem, ahead)
            if step <= second_hops:
                slot = off(step)
                sem = gsem_2 + step * SPLIT + q
                remote(cut(w_g, slot, q), cut(w_g, slot, q), sem - SPLIT, ahead).wait_recv()
                if step < second_hops:
                    start(cut(w_g, slot, q), cut(w_g, slot, q), sem, behind)

    bx_done()
    for i in range(NX):
        for k in range(NZ):
            h, low = k // NZ_LO, k % NZ_LO
            r0, c0 = (h * NX + i) * rows, low * cols
            b_full[r0:r0 + rows, c0:c0 + cols] = b_g[i, k]
    w_all = jnp.concatenate([w_g[i] for i in range(NY)], axis=0)
    result = lax.dot_general(
        b_full[...], w_all, (((1,), (1,)), ((), ())), preferred_element_type=F32
    )
    for i in range(NZ_LO * NC):
        o_f[i] = result[i * rows:(i + 1) * rows]
    for i in range(NZ_LO):
        o_s[pl.ds(i, 1)] = o_f[pl.ds(i * NC + 1 - core, 1)].astype(BF16)
    o_sem = fresh(1)
    start(o_s, o_r, o_sem, at_core)
    remote(o_s, o_r, o_sem, at_core).wait_recv()
    for i in range(NZ_LO):
        f_s[pl.ds(i, 1)] = (
            o_f[pl.ds(i * NC + core, 1)] + o_r[i].astype(F32)[None]
        ).astype(BF16)
    f_r[pl.ds(z_lo, 1)] = f_s[pl.ds(z_lo, 1)]
    f_done = scatter(f_s, f_r, z_lo, NZ_LO, at_zlo)
    f_done()
    for i in range(NZ_LO):
        out[:, i * wide:(i + 1) * wide] = f_r[i].astype(F32)
    for copy in sent:
        copy.wait_send()


def shards(hidden, out_grad, basis_in, basis_out, eigen):
    own_tok, width = hidden.shape
    tokens = out_grad.shape[0]
    inner, depth = basis_in.shape
    rows, cols = basis_out.shape
    wide = width // NZ_LO
    chunk = wide // NY
    half = tokens // NC
    tall, broad = half // 2, depth // 4
    share = tokens // NX
    any_spec = pl.BlockSpec(memory_space=pl.ANY)
    vmem = pltpu.VMEM
    sems = 256
    return pl.pallas_call(
        kernel,
        out_shape=jax.ShapeDtypeStruct((rows, width), F32),
        in_specs=[any_spec] * 5,
        out_specs=pl.BlockSpec(memory_space=pltpu.VMEM),
        scratch_shapes=[
            vmem(hidden.shape, BF16),
            vmem(out_grad.shape, BF16),
            vmem(eigen.shape, F32),
            vmem((NC, inner, depth), BF16),
            vmem((NZ_LO, own_tok, wide), BF16),
            vmem((NZ_LO, own_tok, wide), BF16),
            vmem((NZ, tall, broad), BF16),
            vmem((NZ, tall, broad), BF16),
            vmem((NX, tall, broad), BF16),
            vmem((NZ, tall, broad), BF16),
            vmem((NC, half, depth), BF16),
            vmem((NX, share, cols), BF16),
            vmem((NX, share, cols), BF16),
            vmem((NY, share, cols), BF16),
            vmem((NZ, share, cols), BF16),
            vmem((NX, share, NZ_LO * cols), BF16),
            vmem((NX, NZ, rows, cols), BF16),
            vmem((NX, NZ, rows, cols), BF16),
            vmem((depth, NZ_LO * cols), BF16),
            vmem((NY, chunk, NZ_LO * cols), BF16),
            vmem((NY // 2, chunk, NZ_LO * cols), BF16),
            vmem((NY // 2 - 1, chunk, NZ_LO * cols), BF16),
            vmem((NY, chunk, NZ_LO * cols), BF16),
            vmem((NX * NZ_HI * rows, NZ_LO * cols), BF16),
            vmem((NZ_LO * NC, rows, wide), F32),
            vmem((NZ_LO, rows, wide), BF16),
            vmem((NZ_LO, rows, wide), BF16),
            vmem((NZ_LO, rows, wide), BF16),
            vmem((NZ_LO, rows, wide), BF16),
            pltpu.SemaphoreType.DMA((5,)),
            pltpu.SemaphoreType.DMA((sems,)),
            pltpu.SemaphoreType.DMA((sems,)),
        ],
        compiler_params=pltpu.CompilerParams(collective_id=0, has_side_effects=True),
    )(hidden, out_grad, basis_in, basis_out, eigen)


def solution(mesh):
    placed = (
        P("col", "row"),
        P(None, ("tp", "row")),
        P(("row", "col"), "tp"),
        P(("tp", "row"), "col"),
        P(("tp", "row"), "col"),
    )
    return jax.shard_map(
        shards, mesh=mesh, in_specs=placed, out_specs=P(("tp", "col"), "row"), check_vma=False
    )
```

```python
import functools

import jax
import jax.numpy as jnp
from jax import lax
from jax.experimental import pallas as pl
from jax.experimental.pallas import tpu as pltpu
from jax.sharding import PartitionSpec as P

MESH = pl.DeviceIdType.MESH
BF16 = jnp.bfloat16
F32 = jnp.float32
damping = 0.01
NX, NZ_HI, NZ_LO, NC = 4, 2, 4, 2
NZ = NZ_HI * NZ_LO
NY = 8
PIECES = ((0, 64), (64, 64), (128, 48), (176, 48))
BLOCKS = ((0, 128), (128, 96))


def far_first(count):
    return sorted(range(1, count), key=lambda hop: -min(hop, count - hop))


def kernel(
    hidden, out_grad, basis_in, basis_out, eigen, out,
    hid_v, grad_v, eig_v, basis, hid_s, hid_r,
    p_s, p_r, p_x, p_g, rin,
    r_s, r_r, r_y, r_z, r_x,
    e_g, b_g, rin_t, scaled, w_s, w_1, w_2, w_g, b_full, f_s, f_r,
    load_sem, send_sem, recv_sem,
):
    t = lax.axis_index("tp")
    row = lax.axis_index("row")
    col = lax.axis_index("col")
    z_hi, x = lax.div(row, NX), lax.rem(row, NX)
    z_lo, core = lax.div(col, NC), lax.rem(col, NC)
    z = z_hi * NZ_LO + z_lo

    def at_y(pos):
        return {"tp": pos}

    def at_x(pos):
        return {"row": z_hi * NX + pos}

    def at_z(pos):
        return {
            "row": lax.div(pos, NZ_LO) * NX + x,
            "col": lax.rem(pos, NZ_LO) * NC + core,
        }

    def at_zlo(pos):
        return {"col": pos * NC + core}

    def at_col(pos):
        return {"col": pos}

    at_core = {"col": z_lo * NC + 1 - core}

    slots = [0, 0]
    sent = []

    def fresh(kind, count):
        first = slots[kind]
        slots[kind] += count
        return first

    def remote(src, dst, send, recv, device):
        return pltpu.make_async_remote_copy(
            src_ref=src, dst_ref=dst, send_sem=send_sem.at[send], recv_sem=recv_sem.at[recv],
            device_id=device, device_id_type=MESH,
        )

    def exchange(src, dst, every, me, count, at):
        send, recv = fresh(0, 1), fresh(1, 1)
        for hop in far_first(count):
            peer = lax.rem(me + hop, count)
            remote(src(peer), dst(me), send, recv, at(peer)).start()
        whole = remote(every, every, send, recv, at(lax.rem(me + 1, count)))
        sent.append(whole)
        return whole.wait_recv

    def gather(buf, me, count, at):
        part = buf.at[me]
        return exchange(
            lambda peer: part, lambda mine: part, buf.at[pl.ds(0, count - 1)], me, count, at
        )

    def scatter(src, dst, me, count, at):
        return exchange(
            lambda peer: src.at[peer], lambda mine: dst.at[mine], dst.at[pl.ds(0, count - 1)],
            me, count, at,
        )

    def to_core(ref, other):
        send, recv = fresh(0, 1), fresh(1, 1)
        copy = remote(ref, ref, send, recv, at_core)
        copy.start()
        sent.append(copy)
        return remote(other, other, send, recv, at_core).wait_recv

    def total(buf, count):
        acc = buf[0].astype(F32)
        for i in range(1, count):
            acc = acc + buf[i].astype(F32)
        return acc

    def put(buf, pos, value):
        buf[pl.ds(pos, 1)] = value[None]

    e_own, b_own = e_g.at[core], b_g.at[core]
    loads = [
        pltpu.make_async_copy(hidden, hid_v, load_sem.at[0]),
        pltpu.make_async_copy(out_grad, grad_v, load_sem.at[1]),
        pltpu.make_async_copy(basis_out, b_own.at[x, z], load_sem.at[2]),
        pltpu.make_async_copy(basis_in, basis.at[core], load_sem.at[3]),
        pltpu.make_async_copy(eigen, eig_v, load_sem.at[4]),
    ]
    for load in loads:
        load.start()

    barrier = pltpu.get_barrier_semaphore()
    partners = [at_core]
    partners += [at_x(lax.rem(x + hop, NX)) for hop in range(1, NX)]
    partners += [at_z(lax.rem(z + hop, NZ)) for hop in range(1, NZ)]
    partners += [at_y(lax.rem(t + hop, NY)) for hop in range(1, NY)]
    partners += [
        at_col(lax.rem(z_lo + hop, NZ_LO) * NC + 1 - core) for hop in range(1, NZ_LO)
    ]
    for partner in partners:
        pl.semaphore_signal(barrier, inc=1, device_id=partner, device_id_type=MESH)

    own_tok = hid_v.shape[0]
    wide = hid_s.shape[2]
    loads[0].wait()
    hid = hid_v[...]
    for i in range(NZ_LO):
        hid_s[i] = hid[:, i * wide:(i + 1) * wide]
    hid_r[pl.ds(z_lo, 1)] = hid_s[pl.ds(z_lo, 1)]

    loads[1].wait()
    loads[2].wait()
    part = lax.dot_general(
        grad_v[...], b_g[core, x, z], (((0,), (0,)), ((), ())), preferred_element_type=F32
    )
    order = [i * NC + p for p in range(NC) for i in range(NZ_LO)]
    part = jnp.concatenate([part[i * own_tok:(i + 1) * own_tok] for i in order], axis=0)
    piece = r_s.shape[1]
    for i in range(NX):
        r_s[i] = part[i * piece:(i + 1) * piece].astype(BF16)
    r_r[pl.ds(x, 1)] = r_s[pl.ds(x, 1)]
    loads[3].wait()
    loads[4].wait()
    queries = own_tok * NZ_LO * NC
    e_g[core, x, z] = (1.0 / (queries * (eig_v[...] + damping))).astype(BF16)

    pl.semaphore_wait(barrier, len(partners))

    hid_done = scatter(hid_s, hid_r, z_lo, NZ_LO, at_zlo)
    basis_done = to_core(basis.at[core], basis.at[1 - core])
    r_done = scatter(r_s, r_r, x, NX, at_x)

    def zgather(buf):
        part = buf.at[x, z]
        return exchange(
            lambda peer: part, lambda mine: part, buf.at[x, pl.ds(0, NZ - 1)], z, NZ, at_z
        )

    ez_done = zgather(e_own)

    r_done()
    put(r_y, t, total(r_r, NX).astype(BF16))
    ry_done = gather(r_y, t, NY, at_y)

    hid_done()
    basis_done()
    deep = NC * basis.shape[1]
    depth = basis.shape[2]
    p_full = jnp.dot(
        hid_r[...].reshape(NZ_LO * own_tok, wide), basis[...].reshape(deep, depth),
        preferred_element_type=F32,
    )
    tall, broad = p_s.shape[1:]
    across = depth // broad
    for i in range(NZ):
        h, q = i // across, i % across
        p_s[i] = p_full[h * tall:(h + 1) * tall, q * broad:(q + 1) * broad].astype(BF16)
    p_r[pl.ds(z, 1)] = p_s[pl.ds(z, 1)]
    p_done = scatter(p_s, p_r, z, NZ, at_z)

    ry_done()
    put(r_z, z, total(r_y, NY).astype(BF16))
    rz_done = gather(r_z, z, NZ, at_z)

    p_done()
    put(p_x, x, total(p_r, NZ).astype(BF16))
    px_done = gather(p_x, x, NX, at_x)

    ez_done()
    ex_done = gather(e_own, x, NX, at_x)

    px_done()
    put(p_g, z, total(p_x, NX).astype(BF16))
    pg_done = gather(p_g, z, NZ, at_z)

    rz_done()
    put(
        r_x.at[core], x,
        jnp.concatenate(
            [
                sum(r_z[h * NZ_LO + i].astype(F32) for h in range(NZ_HI)).astype(BF16)
                for i in range(NZ_LO)
            ],
            axis=1,
        ),
    )
    rx_done = gather(r_x.at[core], x, NX, at_x)

    pg_done()
    put(
        rin, core,
        jnp.concatenate(
            [
                jnp.concatenate([p_g[h * across + q] for q in range(across)], axis=1)
                for h in range(NZ // across)
            ],
            axis=0,
        ),
    )
    rin_done = to_core(rin.at[core], rin.at[1 - core])
    rx_done()
    ro_done = to_core(r_x.at[core], r_x.at[1 - core])
    ex_done()
    e_done = to_core(e_own, e_g.at[1 - core])
    bz_done = zgather(b_own)

    rin_done()
    rin_t[...] = rin[...].reshape(queries, depth).T
    ro_done()
    e_done()

    rows, cols = b_g.shape[3:]
    inner = basis.shape[1]
    heading = 1 - 2 * core
    ahead = at_y(lax.rem(t + heading + NY, NY))
    behind = at_y(lax.rem(t - heading + NY, NY))
    first_hops, second_hops = NY // 2, NY // 2 - 1

    def off(steps):
        return lax.rem(t + heading * steps + 2 * NY, NY)

    own_basis = basis[core]

    def form(dest):
        low, par = lax.div(dest, NC), lax.rem(dest, NC)
        lanes = pl.ds(pl.multiple_of(low * cols, cols), cols)
        coeff = jnp.dot(
            rin_t[...], r_x[par, :, :, lanes].reshape(queries, cols), preferred_element_type=F32
        )
        for h in range(NZ_HI):
            for i in range(NX):
                r0 = (h * NX + i) * rows
                scaled[r0:r0 + rows] = (
                    coeff[r0:r0 + rows] * e_g[par, i, h * NZ_LO + low].astype(F32)
                ).astype(BF16)
        put(
            w_s, dest,
            jnp.dot(own_basis, scaled[...], preferred_element_type=F32).astype(BF16),
        )

    count = len(PIECES)

    def cut(buf, slot, q):
        return buf.at[slot, pl.ds(*PIECES[q])]

    def add_in(slot, buf, step, q):
        here = (pl.ds(slot, 1), pl.ds(*PIECES[q]))
        there = (pl.ds(step, 1), pl.ds(*PIECES[q]))
        w_s[here] = (w_s[here].astype(F32) + buf[there].astype(F32)).astype(BF16)

    ring = fresh(0, 1)
    sem_1 = fresh(1, first_hops * count)
    sem_2 = fresh(1, second_hops * count)

    def arrive_1(step, q):
        slot = cut(w_1, step, q)
        remote(slot, slot, ring, sem_1 + step * count + q, behind).wait_recv()

    def arrive_2(step, q):
        slot = cut(w_2, step, q)
        remote(slot, slot, ring, sem_2 + step * count + q, ahead).wait_recv()

    def leave_1(dest, step, q):
        remote(
            cut(w_s, dest, q), cut(w_1, step, q), ring, sem_1 + step * count + q, ahead
        ).start()

    def leave_2(dest, step, q):
        remote(
            cut(w_s, dest, q), cut(w_2, step, q), ring, sem_2 + step * count + q, behind
        ).start()

    form(off(first_hops))
    for q in range(count):
        leave_1(off(first_hops), 0, q)
    form(off(-second_hops))
    for q in range(count):
        leave_2(off(-second_hops), 0, q)
    for step in range(first_hops - 1, 0, -1):
        form(off(step))
        if step > 1:
            form(off(1 - step))
    form(t)
    for step in range(1, first_hops):
        for q in range(count):
            dest = off(first_hops - step)
            arrive_1(step - 1, q)
            add_in(dest, w_1, step - 1, q)
            leave_1(dest, step, q)
            if step < second_hops:
                dest = off(step - second_hops)
                arrive_2(step - 1, q)
                add_in(dest, w_2, step - 1, q)
                leave_2(dest, step, q)
    sent.append(
        remote(
            w_s.at[pl.ds(0, NY - 1)], w_s.at[pl.ds(0, NY - 1)], ring, sem_1, ahead
        )
    )
    bz_done()
    bx_done = gather(b_own, x, NX, at_x)

    round_ = fresh(0, 1)
    gsem_1 = fresh(1, first_hops * count)
    gsem_2 = fresh(1, second_hops * count)

    def pass_on(slot, sem, q, device):
        return remote(cut(w_g, slot, q), cut(w_g, slot, q), round_, sem + q, device)

    for q in range(count):
        arrive_2(second_hops - 1, q)
        add_in(t, w_2, second_hops - 1, q)
        arrive_1(first_hops - 1, q)
        here = (pl.ds(t, 1), pl.ds(*PIECES[q]))
        there = (pl.ds(first_hops - 1, 1), pl.ds(*PIECES[q]))
        w_g[here] = (w_s[here].astype(F32) + w_1[there].astype(F32)).astype(BF16)
        pass_on(t, gsem_1, q, ahead).start()
        pass_on(t, gsem_2, q, behind).start()
    bx_done()
    b_done = to_core(b_own, b_g.at[1 - core])
    for step in range(1, first_hops + 1):
        if step == first_hops:
            b_done()
            for p in range(NC):
                for i in range(NX):
                    for k in range(NZ):
                        h, low = k // NZ_LO, k % NZ_LO
                        r0, c0 = (h * NX + i) * rows, (low * NC + p) * cols
                        b_full[r0:r0 + rows, c0:c0 + cols] = b_g[p, i, k]
        for q in range(count):
            slot = off(-step)
            pass_on(slot, gsem_1 + (step - 1) * count, q, behind).wait_recv()
            if step < first_hops:
                pass_on(slot, gsem_1 + step * count, q, ahead).start()
            if step <= second_hops:
                slot = off(step)
                pass_on(slot, gsem_2 + (step - 1) * count, q, ahead).wait_recv()
                if step < second_hops:
                    pass_on(slot, gsem_2 + step * count, q, behind).start()
    sent.append(
        remote(
            w_g.at[pl.ds(0, NY - 1)], w_g.at[pl.ds(0, NY - 1)], round_, gsem_1, ahead
        )
    )

    f_done = []
    for n, (f0, size) in enumerate(BLOCKS):
        w_all = jnp.concatenate([w_g[i, f0:f0 + size] for i in range(NY)], axis=1)
        result = lax.dot_general(
            b_full[...], w_all, (((1,), (1,)), ((), ())), preferred_element_type=F32
        ).astype(BF16)
        for i in range(NZ_LO * NC):
            f_s[n, i, :, :size] = result[i * rows:(i + 1) * rows]
        f_r[n, pl.ds(col, 1)] = f_s[n, pl.ds(col, 1)]
        f_done.append(scatter(f_s.at[n], f_r.at[n], col, NZ_LO * NC, at_col))
    for n, (f0, size) in enumerate(BLOCKS):
        f_done[n]()
        for i in range(NZ_LO * NC):
            out[:, i * inner + f0:i * inner + f0 + size] = f_r[n, i, :, :size].astype(F32)
    for copy in sent:
        copy.wait_send()


def shards(hidden, out_grad, basis_in, basis_out, eigen):
    out_grad = out_grad.T
    own_tok, width = hidden.shape
    tokens = out_grad.shape[1]
    inner, depth = basis_in.shape
    rows, cols = basis_out.shape
    wide = width // NZ_LO
    half = tokens // NC
    tall, broad = half // 2, depth // 4
    share = tokens // NX
    every = NC * NZ_LO * cols
    any_spec = pl.BlockSpec(memory_space=pl.ANY)
    vmem = pltpu.VMEM
    return pl.pallas_call(
        kernel,
        out_shape=jax.ShapeDtypeStruct((rows, width), F32),
        in_specs=[any_spec] * 5,
        out_specs=pl.BlockSpec(memory_space=pltpu.VMEM),
        scratch_shapes=[
            vmem(hidden.shape, BF16),
            vmem(out_grad.shape, BF16),
            vmem(eigen.shape, F32),
            vmem((NC, inner, depth), BF16),
            vmem((NZ_LO, own_tok, wide), BF16),
            vmem((NZ_LO, own_tok, wide), BF16),
            vmem((NZ, tall, broad), BF16),
            vmem((NZ, tall, broad), BF16),
            vmem((NX, tall, broad), BF16),
            vmem((NZ, tall, broad), BF16),
            vmem((NC, half, depth), BF16),
            vmem((NX, share, cols), BF16),
            vmem((NX, share, cols), BF16),
            vmem((NY, share, cols), BF16),
            vmem((NZ, share, cols), BF16),
            vmem((NC, NX, share, NZ_LO * cols), BF16),
            vmem((NC, NX, NZ, rows, cols), BF16),
            vmem((NC, NX, NZ, rows, cols), BF16),
            vmem((depth, tokens), BF16),
            vmem((depth, cols), BF16),
            vmem((NY, inner, cols), BF16),
            vmem((NY // 2, inner, cols), BF16),
            vmem((NY // 2 - 1, inner, cols), BF16),
            vmem((NY, inner, cols), BF16),
            vmem((NX * NZ_HI * rows, every), BF16),
            vmem((len(BLOCKS), NZ_LO * NC, rows, BLOCKS[0][1]), BF16),
            vmem((len(BLOCKS), NZ_LO * NC, rows, BLOCKS[0][1]), BF16),
            pltpu.SemaphoreType.DMA((5,)),
            pltpu.SemaphoreType.DMA((24,)),
            pltpu.SemaphoreType.DMA((24 + 2 * (NY - 1) * len(PIECES),)),
        ],
        compiler_params=pltpu.CompilerParams(collective_id=0, has_side_effects=True),
    )(hidden, out_grad, basis_in, basis_out, eigen)


def solution(mesh):
    placed = (
        P("col", "row"),
        P(None, ("tp", "row")),
        P(("row", "col"), "tp"),
        P(("tp", "row"), "col"),
        P(("tp", "row"), "col"),
    )
    return jax.shard_map(
        shards, mesh=mesh, in_specs=placed, out_specs=P(("tp", "col"), "row"), check_vma=False
    )
```
